32 devices in a mesh: dp: 4 (over x, y), sp: 8 (over z, core).
Axes of the slice: x: 2, y: 2, z: 4, core: 2. Of those that a mesh axis runs over, the one named last changes fastest.
Arguments:
- hidden: bfloat16 [24, 1024, 3072], P('dp', 'sp'), parts along dimension 0
- cond_vec: bfloat16 [24, 3072], P('dp'), parts along dimension 0
- pos_ids: int32 [1024, 3], P('sp')
- w_mod: bfloat16 [2, 3072, 9216], replicated
- b_mod: bfloat16 [2, 9216], replicated
- w_in: bfloat16 [2, 3072, 21504], replicated
- b_in: bfloat16 [2, 21504], replicated
- q_gain: bfloat16 [2, 128], replicated
- k_gain: bfloat16 [2, 128], replicated
- w_out: bfloat16 [2, 15360, 3072], replicated
- b_out: bfloat16 [2, 3072], replicated
Outputs:
- output: bfloat16 [24, 1024, 3072], P('dp', 'sp'), parts along dimension 0
There are 4 independent parts. The reference program is written for one: setup_inputs(seed, part) draws one part's arguments, and reference() takes and returns one part's arrays. A program takes and returns all parts, laid end to end along the dimension named above; an argument that names none is the same for every part.
All inputs are finite; a program needn't handle non-finite values.
Results may differ from the reference program's by a relative error of at most 0.0114074.
Values are sent between devices in bfloat16 or wider.
A program may use at most 2.25 GiB of HBM per device.

```python
import math
import jax
import jax.numpy as jnp
from jax import lax

BATCH = 6
TEXT_LEN = 512
IMG_LEN = 512
D = 3072
HEADS = 24
HEAD = 128
MLP_DIM = 12288
BLOCKS = 2
QUERY_ROWS = 256

SEQ_LEN = TEXT_LEN + IMG_LEN
ROPE_SPLIT = (16, 56, 56)
ROPE_THETA = 10000.0
NORM_EPS = 1e-6


def image_ids(rng_key):
    half_log = int(math.log2(IMG_LEN)) // 2
    widths = jnp.array([2 ** (half_log - 1), 2 ** half_log, 2 ** (half_log + 1)], dtype=jnp.int32)
    k_width, k_row, k_col = jax.random.split(rng_key, 3)
    grid_width = widths[jax.random.randint(k_width, (), 0, 3)]
    row_off = jax.random.randint(k_row, (), 0, 64)
    col_off = jax.random.randint(k_col, (), 0, 64)
    img_index = jnp.arange(IMG_LEN, dtype=jnp.int32)
    img_ids = jnp.stack([jnp.zeros_like(img_index), row_off + img_index // grid_width, col_off + img_index % grid_width], axis=1)
    return jnp.concatenate([jnp.zeros((TEXT_LEN, 3), jnp.int32), img_ids.astype(jnp.int32)], axis=0)


def setup_inputs(seed: int = 0, part: int = 0) -> dict:
    shared = jax.random.split(jax.random.key(seed), 9)
    part_key = jax.random.fold_in(jax.random.key(seed + 1), part)
    k_text, k_img, k_mean, k_cond = jax.random.split(part_key, 4)
    text_mean = jax.random.normal(k_mean, (D,), jnp.float32)
    text_rows = 0.6 * jax.random.normal(k_text, (BATCH, TEXT_LEN, D), jnp.float32) + text_mean
    img_rows = jax.random.normal(k_img, (BATCH, IMG_LEN, D), jnp.float32)
    hidden = jnp.concatenate([text_rows, img_rows], axis=1).astype(jnp.bfloat16)
    cond_vec = jax.random.normal(k_cond, (BATCH, D), jnp.float32).astype(jnp.bfloat16)
    pos_ids = image_ids(shared[0])
    w_mod = (jax.random.normal(shared[1], (BLOCKS, D, 3 * D), jnp.float32) * D ** -0.5).astype(jnp.bfloat16)
    b_mod = (0.3 * jax.random.normal(shared[2], (BLOCKS, 3 * D), jnp.float32)).astype(jnp.bfloat16)
    w_in = (jax.random.normal(shared[3], (BLOCKS, D, 3 * D + MLP_DIM), jnp.float32) * D ** -0.5).astype(jnp.bfloat16)
    b_in = (0.3 * jax.random.normal(shared[4], (BLOCKS, 3 * D + MLP_DIM), jnp.float32)).astype(jnp.bfloat16)
    q_gain = jax.random.uniform(shared[5], (BLOCKS, HEAD), jnp.float32, 0.8, 2.2).astype(jnp.bfloat16)
    k_gain = jax.random.uniform(shared[6], (BLOCKS, HEAD), jnp.float32, 0.8, 2.2).astype(jnp.bfloat16)
    w_out = (jax.random.normal(shared[7], (BLOCKS, D + MLP_DIM, D), jnp.float32) * (D + MLP_DIM) ** -0.5).astype(jnp.bfloat16)
    b_out = (0.3 * jax.random.normal(shared[8], (BLOCKS, D), jnp.float32)).astype(jnp.bfloat16)
    return dict(hidden=hidden, cond_vec=cond_vec, pos_ids=pos_ids, w_mod=w_mod, b_mod=b_mod, w_in=w_in, b_in=b_in, q_gain=q_gain, k_gain=k_gain, w_out=w_out, b_out=b_out)


def rope_tables(pos_ids):
    angle_parts = []
    for column, rope_dim in enumerate(ROPE_SPLIT):
        inv_freq = 1.0 / (ROPE_THETA ** (jnp.arange(0, rope_dim, 2, dtype=jnp.float32) / rope_dim))
        angle_parts.append(pos_ids[:, column:column + 1].astype(jnp.float32) * inv_freq)
    angles = jnp.concatenate(angle_parts, axis=1)
    return jnp.cos(angles), jnp.sin(angles)


def rms_norm(tensor, gain):
    sq_mean = jnp.mean(tensor * tensor, axis=-1, keepdims=True)
    return tensor * lax.rsqrt(sq_mean + NORM_EPS) * gain.astype(jnp.float32)


def apply_rope(tensor, cos_t, sin_t):
    paired = tensor.reshape(tensor.shape[:-1] + (tensor.shape[-1] // 2, 2))
    even_v = paired[..., 0]
    odd_v = paired[..., 1]
    cos_b = cos_t[:, None, :]
    sin_b = sin_t[:, None, :]
    rotated = jnp.stack([even_v * cos_b - odd_v * sin_b, even_v * sin_b + odd_v * cos_b], axis=-1)
    return rotated.reshape(tensor.shape)


def attention(queries, keys_all, values_all):
    key_f = keys_all.astype(jnp.float32)
    val_f = values_all.astype(jnp.float32)
    q_blocks = queries.reshape(SEQ_LEN // QUERY_ROWS, QUERY_ROWS, HEADS, HEAD)

    def one_block(q_blk):
        scores = jnp.einsum('qhd,khd->hqk', q_blk.astype(jnp.float32), key_f) * HEAD ** -0.5
        probs = jax.nn.softmax(scores, axis=-1)
        return jnp.einsum('hqk,khd->qhd', probs, val_f)

    return lax.map(one_block, q_blocks).reshape(SEQ_LEN, HEADS, HEAD).astype(jnp.bfloat16)


def single_block(hidden, cond_row, cos_t, sin_t, params):
    w_mod, b_mod, w_in, b_in, q_gain, k_gain, w_out, b_out = params
    mod_act = jax.nn.silu(cond_row.astype(jnp.float32)).astype(jnp.bfloat16)
    mod_vals = jnp.dot(mod_act[None, :], w_mod, preferred_element_type=jnp.float32)[0] + b_mod.astype(jnp.float32)
    mod_vals = mod_vals.astype(jnp.bfloat16).astype(jnp.float32)
    mod_shift = mod_vals[:D]
    mod_scale = mod_vals[D:2 * D]
    mod_gate = mod_vals[2 * D:]
    x_float = hidden.astype(jnp.float32)
    centered = x_float - jnp.mean(x_float, axis=-1, keepdims=True)
    normed = centered * lax.rsqrt(jnp.mean(centered * centered, axis=-1, keepdims=True) + NORM_EPS)
    modded = ((1.0 + mod_scale) * normed + mod_shift).astype(jnp.bfloat16)
    proj_in = (jnp.dot(modded, w_in, preferred_element_type=jnp.float32) + b_in.astype(jnp.float32)).astype(jnp.bfloat16)
    q_raw = proj_in[:, :D].reshape(SEQ_LEN, HEADS, HEAD).astype(jnp.float32)
    k_raw = proj_in[:, D:2 * D].reshape(SEQ_LEN, HEADS, HEAD).astype(jnp.float32)
    v_heads = proj_in[:, 2 * D:3 * D].reshape(SEQ_LEN, HEADS, HEAD)
    q_heads = apply_rope(rms_norm(q_raw, q_gain), cos_t, sin_t).astype(jnp.bfloat16)
    k_heads = apply_rope(rms_norm(k_raw, k_gain), cos_t, sin_t).astype(jnp.bfloat16)
    attn_out = attention(q_heads, k_heads, v_heads).reshape(SEQ_LEN, D)
    mlp_act = jax.nn.gelu(proj_in[:, 3 * D:].astype(jnp.float32), approximate=True).astype(jnp.bfloat16)
    joined = jnp.concatenate([attn_out, mlp_act], axis=1)
    block_out = (jnp.dot(joined, w_out, preferred_element_type=jnp.float32) + b_out.astype(jnp.float32)).astype(jnp.bfloat16)
    return (x_float + mod_gate * block_out.astype(jnp.float32)).astype(jnp.bfloat16)


def reference(hidden, cond_vec, pos_ids, w_mod, b_mod, w_in, b_in, q_gain, k_gain, w_out, b_out):
    cos_t, sin_t = rope_tables(pos_ids)
    stacked = (w_mod, b_mod, w_in, b_in, q_gain, k_gain, w_out, b_out)

    def one_item(item_pair):
        tokens, cond_row = item_pair

        def layer_step(state, params):
            return single_block(state, cond_row, cos_t, sin_t, params), None

        final_x, _ = lax.scan(layer_step, tokens, stacked)
        return final_x

    return lax.map(one_item, (hidden, cond_vec))
```

```python
import functools
import math
import jax
import jax.numpy as jnp
from jax import lax
from jax.experimental import pallas as pl
from jax.experimental.pallas import tpu as pltpu
from jax.sharding import PartitionSpec as P

HEAD = 128
ROPE_SPLIT = (16, 56, 56)
ROPE_THETA = 10000.0
NORM_EPS = 1e-6
RB = 128
LOG2E = 1.4426950408889634
BF = jnp.bfloat16
F32 = jnp.float32
VMEM_LIMIT = 62 * 2 ** 20


def params(**kw):
    return pltpu.CompilerParams(vmem_limit_bytes=VMEM_LIMIT, **kw)


def cost(flops, nbytes, trans=0):
    return pl.CostEstimate(flops=int(flops), bytes_accessed=int(nbytes), transcendentals=int(trans))


def mod_body(me_ref, c_ref, w_ref, b_ref, o_ref):
    act = c_ref[...].astype(F32)
    act = (act * jax.nn.sigmoid(act)).astype(BF)
    y = jnp.dot(act, w_ref[...], preferred_element_type=F32)
    o_ref[...] = (y + b_ref[...].astype(F32)).astype(BF).astype(F32)


def modulation_part(me, cond8, w_mod, b_mod, n_shards):
    n_layers, d, width = w_mod.shape
    part = width // n_shards
    tile = 384
    steps = part // tile
    return pl.pallas_call(
        mod_body,
        grid_spec=pltpu.PrefetchScalarGridSpec(
            num_scalar_prefetch=1,
            grid=(n_layers, steps),
            in_specs=[
                pl.BlockSpec((8, d), lambda l, i, me: (0, 0)),
                pl.BlockSpec((None, d, tile), lambda l, i, me: (l, 0, me[0] * steps + i)),
                pl.BlockSpec((None, 1, tile), lambda l, i, me: (l, 0, me[0] * steps + i)),
            ],
            out_specs=pl.BlockSpec((None, 8, tile), lambda l, i, me: (l, 0, i)),
        ),
        out_shape=jax.ShapeDtypeStruct((n_layers, 8, part), F32),
        name="mod",
        compiler_params=params(),
        cost_estimate=cost(2 * 8 * d * part * n_layers, n_layers * d * part * 2),
    )(me.reshape(1), cond8, w_mod, b_mod.reshape(n_layers, 1, width))


def ln_body(counts, items, *refs):
    xs, (sh_ref, sc_ref), u_ref = refs[:len(counts)], refs[len(counts):len(counts) + 2], refs[-1]
    i = pl.program_id(0)
    first = 0
    for x_ref, n, it in zip(xs, counts, items):
        @pl.when((i >= first) & (i < first + n))
        def _(x_ref=x_ref, it=it):
            x = x_ref[...].astype(F32)
            cen = x - jnp.mean(x, axis=-1, keepdims=True)
            var = jnp.mean(cen * cen, axis=-1, keepdims=True)
            nrm = cen * lax.rsqrt(var + NORM_EPS)
            u_ref[...] = ((1.0 + sc_ref[it:it + 1, :]) * nrm + sh_ref[it:it + 1, :]).astype(BF)
        first += n


def layer_norm(xs, items, shift, scale, after=()):
    counts = [x.shape[0] for x in xs]
    _, rb, d = xs[0].shape
    nb = sum(counts)
    firsts = [sum(counts[:n]) for n in range(len(counts))]
    x_specs = [pl.BlockSpec((None, rb, d), functools.partial(lambda f, n, i: (jnp.clip(i - f, 0, n - 1), 0, 0), f, n))
               for f, n in zip(firsts, counts)]
    return pl.pallas_call(
        functools.partial(ln_body, counts, items),
        grid=(nb,),
        in_specs=x_specs + [pl.BlockSpec((2, d), lambda i: (0, 0))] * 2 + [pl.BlockSpec(memory_space=pl.ANY)] * len(after),
        out_specs=pl.BlockSpec((None, rb, d), lambda i: (i, 0, 0)),
        out_shape=jax.ShapeDtypeStruct((nb, rb, d), BF),
        name="ln",
        compiler_params=params(),
        cost_estimate=cost(2000 * nb * rb * d, nb * rb * d * 4),
    )(*xs, shift, scale, *after)


def gelu(x):
    c = 0.7978845608028654
    x2 = x * x
    t = x * (x2 * (c * 0.044715) + c)
    h = 0.5 * x
    return h * jnp.tanh(t) + h


def rope_head(h, gain, cos, sin, even):
    ms = jnp.mean(h * h, axis=-1, keepdims=True)
    t = h * lax.rsqrt(ms + NORM_EPS) * gain
    sw = jnp.where(even, pltpu.roll(t, HEAD - 1, 1), pltpu.roll(t, 1, 1))
    return t * cos + sw * sin


def in_body(layer, n_first, kinds, place, tabs, tn, u_ref, w_ref, b_ref, g_ref, cos_ref, sin_ref, *rest):
    outs, acc = rest[:-1], rest[-1]
    step = pl.program_id(0)
    n_steps = pl.num_programs(0) - 1
    n_blocks = len(place)
    groups = [list(range(b, min(b + 2, n_blocks))) for b in range(0, n_blocks, 2)]
    unit = 256

    def epilogue(kind, pair, group, j):
        c0 = j * unit
        for b in group:
            which, slot = place[b]
            out = outs[2 * pair + which]
            r0 = b * RB
            a = acc[r0:r0 + RB, c0:c0 + unit] + b_ref[layer:layer + 1, c0:c0 + unit]
            if kind == "v":
                out[slot, :, c0:c0 + unit] = a.astype(BF)
            elif kind == "m":
                out[slot, :, c0:c0 + unit] = gelu(a.astype(BF).astype(F32)).astype(BF)
            else:
                h = a.astype(BF).astype(F32)
                even = lax.broadcasted_iota(jnp.int32, (RB, HEAD), 1) % 2 == 0
                for s in range(unit // HEAD):
                    y = rope_head(h[:, s * HEAD:(s + 1) * HEAD], g_ref[...], cos_ref[tabs[b]], sin_ref[tabs[b]], even)
                    out[slot, :, c0 + s * HEAD:c0 + (s + 1) * HEAD] = y.astype(BF)

    def emit(kind, pair, with_dot):
        for group in groups:
            r0, rows = group[0] * RB, len(group) * RB
            for j in range(tn // unit):
                if kind is not None:
                    epilogue(kind, pair, group, j)
            if with_dot:
                lhs = u_ref[group[0]:group[0] + len(group)].reshape(rows, u_ref.shape[-1])
                for j in range(tn // unit):
                    acc[r0:r0 + rows, j * unit:(j + 1) * unit] = jnp.dot(
                        lhs, w_ref[:, j * unit:(j + 1) * unit], preferred_element_type=F32)

    first, second = kinds

    @pl.when(step == 0)
    def _():
        emit(None, 0, True)

    @pl.when((step > 0) & (step <= n_first))
    def _():
        emit(first, 0, True)

    @pl.when((step > n_first) & (step < n_steps))
    def _():
        emit(second, 1, True)

    @pl.when(step == n_steps)
    def _():
        emit(second, 1, False)


def in_proj(layer, u, w_in, b_in, gain, cos, sin, place, tabs, sizes, parts, tn, aliased, name, after=()):
    n_blocks, rb, d = u.shape
    rows = n_blocks * rb
    (c0, w0, k0), (c1, w1, k1) = parts
    n0, n1 = w0 // tn, w1 // tn
    o0, o1 = c0 // tn, c1 // tn
    steps = n0 + n1

    def col(i):
        j = jnp.minimum(i, steps - 1)
        return jnp.where(j < n0, o0 + j, o1 + j - n0)

    def lag(i):
        return col(jnp.maximum(i - 1, 0))

    def out0(i):
        return jnp.clip(i - 1, 0, n0 - 1)

    def out1(i):
        return jnp.clip(i - 1 - n0, 0, n1 - 1)

    slots = [[s for w, s in place if w == it] for it in (0, 1)]
    out_shapes, out_specs, out_fns = [], [], (out0, out1)
    local_place = [(w, s - min(slots[w])) for w, s in place]
    for p, width in enumerate((w0, w1)):
        for it in (0, 1):
            n = len(slots[it]) or 1
            base = (min(slots[it]) // n) if slots[it] else 0
            out_shapes.append(jax.ShapeDtypeStruct((sizes[it], rb, width), BF))
            out_specs.append(pl.BlockSpec((n, rb, tn), functools.partial(lambda f, base, i: (base, 0, f(i)), out_fns[p], base)))
    keep = [o for o in range(4) if slots[o % 2]]
    idx = {o: n for n, o in enumerate(keep)}
    n_alias = len(keep) if aliased is not None else 0
    alias_in = [aliased[o] for o in keep] if aliased is not None else []

    def body(*refs):
        ins, rest = refs[:6], refs[6:]
        outs, acc = rest[-1 - len(keep):-1], rest[-1]
        full = [outs[idx[o]] if o in idx else None for o in range(4)]
        in_body(layer, n0, (k0, k1), local_place, tabs, tn, *ins, *full, acc)

    res = pl.pallas_call(
        body,
        grid=(steps + 1,),
        in_specs=[
            pl.BlockSpec((n_blocks, rb, d), lambda i: (0, 0, 0)),
            pl.BlockSpec((None, d, tn), lambda i: (layer, 0, col(i))),
            pl.BlockSpec((2, tn), lambda i: (0, lag(i))),
            pl.BlockSpec((1, HEAD), lambda i: (0, 0)),
            pl.BlockSpec(cos.shape, lambda i: (0, 0, 0)),
            pl.BlockSpec(sin.shape, lambda i: (0, 0, 0)),
        ] + [pl.BlockSpec(memory_space=pl.ANY)] * (n_alias + len(after)),
        out_specs=[out_specs[o] for o in keep],
        out_shape=[out_shapes[o] for o in keep],
        scratch_shapes=[pltpu.VMEM((rows, tn), F32)],
        input_output_aliases={6 + n: n for n in range(n_alias)},
        name=name,
        compiler_params=params(),
        cost_estimate=cost(2 * rows * d * (w0 + w1), (w0 + w1) * (d + rows) * 2, rows * w1),
    )(u, w_in, b_in, gain, cos, sin, *alias_in, *after)
    full = list(aliased) if aliased is not None else [None] * 4
    for o, r in zip(keep, res):
        full[o] = r
    return full


def attn_body(n_kv, heads, q_ref, *refs):
    ks, vs, o_ref = refs[:n_kv], refs[n_kv:2 * n_kv], refs[2 * n_kv]
    qb = q_ref.shape[0]
    c = HEAD ** -0.5 * LOG2E
    for h in range(heads):
        cols = slice(h * HEAD, (h + 1) * HEAD)
        for b in range(0, qb, 2):
            q = q_ref[b:b + 2, :, cols].reshape(2 * RB, HEAD)
            ss = []
            for k_ref in ks:
                k = k_ref[:, :, cols].reshape(-1, HEAD)
                ss.append(lax.dot_general(q, k, (((1,), (1,)), ((), ())), preferred_element_type=F32))
            m = functools.reduce(jnp.maximum, [jnp.max(s, axis=-1, keepdims=True) for s in ss])
            total, o = None, None
            for s, v_ref in zip(ss, vs):
                p = jnp.exp2((s - m) * c)
                t = jnp.sum(p, axis=-1, keepdims=True)
                v = v_ref[:, :, cols].reshape(-1, HEAD)
                d = jnp.dot(p.astype(BF), v, preferred_element_type=F32)
                total = t if total is None else total + t
                o = d if o is None else o + d
            o_ref[b:b + 2, :, cols] = (o / total).astype(BF).reshape(2, RB, HEAD)


def attention(q, kvs, heads_per_step, name):
    qb, rb, d = q.shape
    w = heads_per_step * HEAD
    n_kv = len(kvs)
    spec = lambda n: pl.BlockSpec((n, rb, w), lambda i: (0, 0, i))
    keys = [k for k, _ in kvs]
    vals = [v for _, v in kvs]
    n_keys = sum(k.shape[0] for k in keys) * rb
    return pl.pallas_call(
        functools.partial(attn_body, n_kv, heads_per_step),
        grid=(d // w,),
        in_specs=[spec(qb)] + [spec(k.shape[0]) for k in keys] + [spec(v.shape[0]) for v in vals],
        out_specs=spec(qb),
        out_shape=jax.ShapeDtypeStruct((qb, rb, d), BF),
        name=name,
        compiler_params=params(),
        cost_estimate=cost(8 * qb * rb * n_keys * d, 2 * d * rb * (2 * qb) + 4 * d * n_keys, qb * rb * n_keys * (d // HEAD)),
    )(q, *keys, *vals)


def out_body(layer, items, counts, n_x, n_m, tk, *refs):
    n_src = len(items)
    m_refs, o_refs = refs[:n_src], refs[n_src:2 * n_src]
    w_ref, b_ref, gate_ref = refs[2 * n_src:2 * n_src + 3]
    x_refs = refs[2 * n_src + 3:2 * n_src + 3 + n_x]
    outs, acc = refs[-1 - n_src:-1], refs[-1]
    step = pl.program_id(0)
    last = pl.num_programs(0) - 1
    n = w_ref.shape[-1]
    unit = 256

    @pl.when(step == 0)
    def _():
        acc[...] = jnp.zeros_like(acc)

    def accumulate(srcs):
        blocks = [src.at[b] for src in srcs for b in range(src.shape[0])]
        for p in range(0, len(blocks), 2):
            lhs = jnp.concatenate([blk[...] for blk in blocks[p:p + 2]], axis=0)
            r0, r1 = p * RB, p * RB + lhs.shape[0]
            for j in range(n // unit):
                acc[r0:r1, j * unit:(j + 1) * unit] += jnp.dot(
                    lhs, w_ref[:, j * unit:(j + 1) * unit], preferred_element_type=F32)

    @pl.when(step < n_m)
    def _():
        accumulate(m_refs)

    @pl.when(step >= n_m)
    def _():
        accumulate(o_refs)

    @pl.when(step == last)
    def _():
        xs = [x_ref.at[b] for x_ref in x_refs for b in range(x_ref.shape[0])]
        r = 0
        for it, nb, out in zip(items, counts, outs):
            for b in range(nb):
                y = (acc[r * RB:(r + 1) * RB, :] + b_ref[layer:layer + 1, :]).astype(BF).astype(F32)
                out[b] = (xs[r][...].astype(F32) + gate_ref[it:it + 1, :] * y).astype(BF)
                r += 1


def out_proj(layer, srcs, xs, w_out, b_out, gate, tk, name):
    d = w_out.shape[-1]
    f = srcs[0][0].shape[-1]
    n_m, n_o = f // tk, d // tk
    nbs = [s[4] for s in srcs]
    rows = sum(nbs) * RB

    def specs(col, width, among):
        return [pl.BlockSpec((nb, RB, width), functools.partial(lambda base, i: (base, 0, col(i)), base // nb)) for base, nb in among]

    rng = [s[3:5] for s in srcs]
    return pl.pallas_call(
        functools.partial(out_body, layer, [s[2] for s in srcs], nbs, len(xs), n_m, tk),
        grid=(n_m + n_o,),
        in_specs=specs(lambda i: jnp.minimum(i, n_m - 1), tk, rng) + specs(lambda i: jnp.maximum(i - n_m, 0), tk, rng) + [
            pl.BlockSpec((None, tk, d), lambda i: (layer, jnp.where(i < n_m, n_o + i, i - n_m), 0)),
            pl.BlockSpec((2, d), lambda i: (0, 0)),
            pl.BlockSpec((2, d), lambda i: (0, 0)),
        ] + specs(lambda i: 0, d, [x[1:] for x in xs]),
        out_specs=[pl.BlockSpec((nb, RB, d), lambda i: (0, 0, 0)) for nb in nbs],
        out_shape=[jax.ShapeDtypeStruct((nb, RB, d), BF) for nb in nbs],
        scratch_shapes=[pltpu.VMEM((rows, d), F32)],
        name=name,
        compiler_params=params(),
        cost_estimate=cost(2 * rows * (d + f) * d, (d + f) * d * 2 + rows * (3 * d + f) * 2),
    )(*[s[0] for s in srcs], *[s[1] for s in srcs], w_out, b_out, gate, *[x[0] for x in xs])


def rope_tables(pos):
    parts = []
    for column, rope_dim in enumerate(ROPE_SPLIT):
        inv_freq = 1.0 / (ROPE_THETA ** (jnp.arange(0, rope_dim, 2, dtype=F32) / rope_dim))
        inv_freq = jnp.repeat(inv_freq, 2)
        parts.append(pos[..., column:column + 1].astype(F32) * inv_freq)
    angles = jnp.concatenate(parts, axis=-1)
    sign = jnp.where(jnp.arange(HEAD) % 2 == 0, -1.0, 1.0).astype(F32)
    return jnp.cos(angles), jnp.sin(angles) * sign


def solution(mesh):
    row_spec = P('dp', 'sp', None)
    rep = P()
    n_sp = mesh.shape['sp']

    def swap_chip(v, d):
        return lax.ppermute(v, 'sp', [(i, ((i // 2) ^ d) * 2 + i % 2) for i in range(n_sp)])

    def swap_core(v):
        return lax.ppermute(v, 'sp', [(i, i ^ 1) for i in range(n_sp)])

    def local_forward(hidden, cond_vec, pos_ids, w_mod, b_mod, w_in, b_in, q_gain, k_gain, w_out, b_out):
        d = hidden.shape[-1]
        f = w_out.shape[1] - d
        me = lax.axis_index('sp')
        z = me // 2
        half = z // 2

        def item(i):
            return lax.dynamic_slice_in_dim(hidden, i, 1, axis=0)

        a1 = swap_chip(item(z ^ 1), 1)
        c2 = swap_chip(item(5 - half), 2)
        a2 = swap_chip(item(z ^ 2), 2)
        a3 = swap_chip(item(z ^ 3), 3)
        pos = jnp.stack([pos_ids, swap_chip(pos_ids, 1), swap_chip(pos_ids, 2), swap_chip(pos_ids, 3)])
        cos_b, sin_b = rope_tables(pos)

        cond8 = jnp.concatenate([cond_vec, jnp.zeros((2, d), cond_vec.dtype)], axis=0)
        mod = modulation_part(me, cond8, w_mod, b_mod, n_sp)
        mod = lax.all_gather(mod, 'sp', axis=0)
        mod = jnp.moveaxis(mod, 0, 2).reshape(mod.shape[1], 8, 3 * d)
        mod = jnp.concatenate([lax.dynamic_slice_in_dim(mod, z, 1, axis=1),
                               lax.dynamic_slice_in_dim(mod, 4 + half, 1, axis=1)], axis=1)
        b_in32 = b_in.astype(F32)
        b_out32 = b_out.astype(F32)
        qg = q_gain.astype(F32)
        kg = k_gain.astype(F32)

        own_a, own_c = item(z), item(4 + half)
        chunks = [
            ((own_a, own_c), (0, 1), (0, 0), [(0, 0), (1, 0)]),
            ((a1, c2), (0, 1), (1, 2), [(0, 1), (1, 1)]),
            ((a2, a3), (0, 0), (2, 3), [(0, 2), (0, 3)]),
        ]
        sizes = (4, 2)
        kv_parts = ((d, d, "qk"), (2 * d, d, "v"))
        qm_parts = ((0, d, "qk"), (3 * d, f, "m"))
        n_layers = w_mod.shape[0]
        xa = xc = None
        for layer in range(n_layers):
            shift, scale, gate = mod[layer, :, :d], mod[layer, :, d:2 * d], mod[layer, :, 2 * d:]
            kg32, qg32 = kg[layer:layer + 1], qg[layer:layer + 1]
            kv = qm = None
            if layer == 0:
                for n, (xs, items, tabs, place) in enumerate(chunks):
                    u = layer_norm(xs, items, shift, scale, qm[2:3] if n else ())
                    kv = in_proj(layer, u, w_in, b_in32, kg32, cos_b, sin_b, place, tabs, sizes, kv_parts, 1024, kv, f"kv{n}")
                    qm = in_proj(layer, u, w_in, b_in32, qg32, cos_b, sin_b, place, tabs, sizes, qm_parts, 1024, qm, f"qm{n}", kv[2:3])
                xs_all = [(own_a, 0, 1), (a1, 0, 1), (a2, 0, 1), (a3, 0, 1), (own_c, 0, 1), (c2, 0, 1)]
            else:
                u = layer_norm((xa, xc), (0, 1), shift, scale)
                tabs = (0, 1, 2, 3, 0, 2)
                place = [(0, 0), (0, 1), (0, 2), (0, 3), (1, 0), (1, 1)]
                kv = in_proj(layer, u, w_in, b_in32, kg32, cos_b, sin_b, place, tabs, sizes, kv_parts, 512, None, "kv")
                qm = in_proj(layer, u, w_in, b_in32, qg32, cos_b, sin_b, place, tabs, sizes, qm_parts, 512, None, "qm", kv[2:3])
            ka, kc, va, vc = kv
            qa, qc, ga, gc = qm
            kc1, vc1 = swap_chip(kc, 1), swap_chip(vc, 1)
            ka_s, va_s = swap_core(ka), swap_core(va)
            kc_s, vc_s = swap_core(kc), swap_core(vc)
            kc1_s, vc1_s = swap_core(kc1), swap_core(vc1)
            oa = attention(qa, [(ka, va), (ka_s, va_s)], 4, "attn_a")
            oc = attention(qc, [(kc, vc), (kc_s, vc_s), (kc1, vc1), (kc1_s, vc1_s)], 4, "attn_c")
            if layer < n_layers - 1:
                xa, xc = out_proj(layer, [(ga, oa, 0, 0, 4), (gc, oc, 1, 0, 2)], xs_all, w_out, b_out32, gate, 512, "out")
            else:
                far2, far3 = out_proj(layer, [(ga, oa, 0, 2, 1), (ga, oa, 0, 3, 1)], [(xa, 2, 2)], w_out, b_out32, gate, 1024, "out_far")
                y2, y3 = swap_chip(far2, 2), swap_chip(far3, 3)
                near_a, near_c = out_proj(layer, [(ga, oa, 0, 1, 1), (gc, oc, 1, 1, 1)], [(xa, 1, 1), (xc, 1, 1)], w_out, b_out32, gate, 1024, "out_near")
                yc2, y1 = swap_chip(near_c, 2), swap_chip(near_a, 1)
                own_a, own_c = out_proj(layer, [(ga, oa, 0, 0, 1), (gc, oc, 1, 0, 1)], [(xa, 0, 1), (xc, 0, 1)], w_out, b_out32, gate, 1024, "out_own")
        out = jnp.zeros_like(hidden)
        for piece, i in ((own_a, z), (y1, z ^ 1), (y2, z ^ 2), (y3, z ^ 3), (own_c, 4 + half), (yc2, 5 - half)):
            out = lax.dynamic_update_slice_in_dim(out, piece, i, axis=0)
        return out

    in_specs = (row_spec, P('dp', None), P('sp', None)) + (rep,) * 8
    return jax.shard_map(local_forward, mesh=mesh, in_specs=in_specs, out_specs=row_spec, check_vma=False)
```
